32 devices in a mesh: blk: 16 (over z, y, core), head: 2 (over x).
Axes of the slice: x: 2, y: 2, z: 4, core: 2. Of those that a mesh axis runs over, the one named last changes fastest.
Arguments:
- tokens: bfloat16 [2048, 3584], P(('blk', 'head')), may hold values from -100 to 100
- norm_gain: float32 [3584], replicated, may hold values from 0.1 to 1.9
- w_query: bfloat16 [3584, 3072], P('blk', 'head'), may hold values from -0.09375 to 0.09375
- w_key: bfloat16 [3584, 512], P('blk'), may hold values from -0.09375 to 0.09375
- w_value: bfloat16 [3584, 512], P('blk'), may hold values from -0.09375 to 0.09375
- q_bias: float32 [3072], P('head'), may hold values from -200 to 200
- k_bias: float32 [512], replicated, may hold values from -25 to 25
- v_bias: float32 [512], replicated, may hold values from -2.5 to 2.5
- w_out: bfloat16 [3072, 3584], P('head', 'blk'), may hold values from -0.109375 to 0.109375
Outputs:
- attention_out: bfloat16 [2048, 3584], P(('blk', 'head'))
The draws below stay inside these ranges and needn't reach their ends.
All inputs are finite; a program needn't handle non-finite values.
Results may differ from the reference program's by a relative error of at most 0.04.
The reference program's roundings to bfloat16 on the way count: a program that leaves them out, or rounds other values in their place, can miss the bound.
Values may be sent and summed in bfloat16 or wider, within the bound.
No kernel may reach another device: no remote copies, remote signals or barrier semaphores. Data moves between devices by JAX's collectives and lax.ppermute only.
A program may use at most 64 MiB of HBM per device.

```python
import jax
import jax.numpy as jnp
from jax import lax

D = 3584
HD = 128
H = 24
G = 6
KVH = 4
SEQ = 2048


def draw_tokens(key, part):
    first, second, third = jax.random.split(jax.random.fold_in(key, 5), 3)
    row_scale = jnp.exp(jax.random.uniform(second, (SEQ, 1), minval=0.0, maxval=jnp.log(10.0)))
    col_scale = jnp.exp(jax.random.uniform(third, (1, D), minval=jnp.log(0.3), maxval=jnp.log(3.0)))
    base = jax.random.normal(first, (SEQ, D))
    return jnp.clip(base * row_scale * col_scale, -100.0, 100.0).astype(jnp.bfloat16)


def draw_q_bias(key, part):
    values = 0.5 * jax.random.normal(jax.random.fold_in(key, 3), (H * HD,))
    return jnp.clip(values, -2.0, 2.0).astype(jnp.float32)


def draw_k_bias(key, part):
    values = 0.5 * jax.random.normal(jax.random.fold_in(key, 4), (KVH * HD,))
    return jnp.clip(values, -2.0, 2.0).astype(jnp.float32)


def shard_levels(key, extent, cuts, least, largest):
    def one(axis_at, shards_of):
        steps = jax.random.uniform(jax.random.fold_in(jax.random.fold_in(key, 6), axis_at), (shards_of,), jnp.float32, least / len(cuts), largest / len(cuts))
        return jnp.repeat(jnp.exp(steps), extent[axis_at] // shards_of).reshape((-1,) + (1,) * (len(extent) - axis_at - 1))

    gain = one(*cuts[0])
    for cut in cuts[1:]:
        gain = gain * one(*cut)
    return gain


def normal_values(key, dims, scale, limit, cuts=(), kind=jnp.bfloat16):
    level = shard_levels(key, dims, cuts, -0.22, 0.18) if cuts else 1.0
    values = jax.random.normal(key, dims, jnp.float32) * scale * level
    return jnp.minimum(jnp.maximum(values, -limit), limit).astype(kind)


def setup_inputs(seed: int = 0) -> dict:
    key_list = jax.random.split(jax.random.key(seed), 10)
    tokens = draw_tokens(jax.random.fold_in(key_list[9], 71), 0)
    norm_gain = jnp.clip(1.0 + 0.18 * jax.random.normal(key_list[1], (D,), jnp.float32), 0.1, 1.9)
    w_query = normal_values(key_list[2], (D, H * HD), D ** -0.5, 0.09375, ((0, 16), (1, 2)))
    w_key = normal_values(key_list[3], (D, KVH * HD), D ** -0.5, 0.09375, ((0, 16),))
    w_value = normal_values(key_list[4], (D, KVH * HD), D ** -0.5, 0.09375, ((0, 16),))
    q_bias = draw_q_bias(jax.random.fold_in(key_list[9], 71), 0)
    k_bias = draw_k_bias(jax.random.fold_in(key_list[9], 71), 0)
    v_bias = normal_values(key_list[7], (KVH * HD,), 0.5, 2.5, (), jnp.float32)
    w_out = normal_values(key_list[8], (H * HD, D), (H * HD) ** -0.5, 0.109375, ((0, 2), (1, 16)))
    return {"tokens": tokens, "norm_gain": norm_gain, "w_query": w_query, "w_key": w_key, "w_value": w_value, "q_bias": q_bias, "k_bias": k_bias, "v_bias": v_bias, "w_out": w_out}


theta_base = 1000000.0
eps_norm = 1e-06
masked_score = -1e+30

def rotary_tables(positions, width):
    half = width // 2
    freq = theta_base ** (-(jnp.arange(half, dtype=jnp.float32) * 2.0 / width))
    angles = positions.astype(jnp.float32)[:, None] * freq[None, :]
    angles = jnp.concatenate([angles, angles], axis=1)
    return (jnp.cos(angles), jnp.sin(angles))

def rotate(values, cosine, sine):
    half = values.shape[-1] // 2
    turned = jnp.concatenate([-values[..., half:], values[..., :half]], axis=-1)
    return values * cosine[:, None, :] + turned * sine[:, None, :]

def reference(tokens, norm_gain, w_query, w_key, w_value, q_bias, k_bias, v_bias, w_out):
    seq_len = tokens.shape[0]
    floats = tokens.astype(jnp.float32)
    normed = (floats * lax.rsqrt(lax.optimization_barrier(jnp.mean(floats * floats, axis=1, keepdims=True)) + eps_norm) * norm_gain).astype(jnp.bfloat16)
    cosine, sine = rotary_tables(jnp.arange(seq_len, dtype=jnp.int32), HD)
    query = jnp.dot(normed, w_query, preferred_element_type=jnp.float32) + q_bias
    query = rotate(query.reshape(seq_len, H, HD), cosine, sine).astype(jnp.bfloat16)
    key = jnp.dot(normed, w_key, preferred_element_type=jnp.float32) + k_bias
    key = rotate(key.reshape(seq_len, KVH, HD), cosine, sine).astype(jnp.bfloat16)
    value = (jnp.dot(normed, w_value, preferred_element_type=jnp.float32) + v_bias).astype(jnp.bfloat16)
    value = value.reshape(seq_len, KVH, HD)
    width = min(512, seq_len)
    block_total = seq_len // width
    scale = 1.0 / HD ** 0.5
    key_positions = jnp.arange(seq_len, dtype=jnp.int32)

    def one_group(group):
        query_group = lax.dynamic_slice_in_dim(query, (group * G).astype(jnp.int32), G, 1)
        key_group = lax.dynamic_index_in_dim(key, group, 1, keepdims=False).astype(jnp.float32)
        value_group = lax.dynamic_index_in_dim(value, group, 1, keepdims=False).astype(jnp.float32)

        def one_block(block):
            start = (block * width).astype(jnp.int32)
            rows_block = lax.dynamic_slice_in_dim(query_group, start, width, 0).astype(jnp.float32)
            scores = jnp.einsum('qhd,kd->hqk', rows_block, key_group) * scale
            query_positions = start + jnp.arange(width, dtype=jnp.int32)
            visible = key_positions[None, :] <= query_positions[:, None]
            scores = jnp.where(visible[None], scores, masked_score)
            top = lax.optimization_barrier(jnp.max(scores, axis=2, keepdims=True))
            weights = jnp.where(visible[None], jnp.exp(scores - top), 0.0)
            total = lax.optimization_barrier(jnp.sum(weights, axis=2))
            rounded = lax.optimization_barrier(weights.astype(jnp.bfloat16))
            mixed = jnp.einsum('hqk,kd->hqd', rounded.astype(jnp.float32), value_group)
            return (mixed / total[..., None]).astype(jnp.bfloat16)
        return lax.map(one_block, jnp.arange(block_total, dtype=jnp.int32))
    outs = lax.map(one_group, jnp.arange(KVH, dtype=jnp.int32))
    attended = outs.transpose(1, 3, 0, 2, 4).reshape(seq_len, H * HD)
    return jnp.dot(attended, w_out, preferred_element_type=jnp.float32).astype(jnp.bfloat16)
```

```python
import math

import jax
import jax.numpy as jnp
from jax import lax
from jax.experimental import pallas as pl
from jax.experimental.pallas import tpu as pltpu
from jax.sharding import PartitionSpec as P

HD = 128
G = 6


theta_base = 1000000.0
eps_norm = 1e-06
masked_score = -1e30


def rotary_tables(positions, width):
    half = width // 2
    freq = theta_base ** (-(jnp.arange(half, dtype=jnp.float32) * 2.0 / width))
    angles = positions.astype(jnp.float32)[:, None] * freq[None, :]
    angles = jnp.concatenate([angles, angles], axis=1)
    return (jnp.cos(angles), jnp.sin(angles))


def rotate(values, cosine, sine):
    half = values.shape[-1] // 2
    turned = jnp.concatenate([-values[..., half:], values[..., :half]], axis=-1)
    return values * cosine[:, None, :] + turned * sine[:, None, :]


def block_width(rows, limit):
    width = min(rows, limit)
    while rows % width:
        width -= 1
    return width


def on_device_plain(tokens, norm_gain, w_query, w_key, w_value, q_bias, k_bias, v_bias, w_out):
    head_count = lax.axis_size("head")
    head_index = lax.axis_index("head")
    block_index = lax.axis_index("blk")
    local_rows = tokens.shape[0]
    group_rows = local_rows * head_count
    heads_here = w_query.shape[1] // HD
    kv_here = max(1, heads_here // G)
    per_kv = heads_here // kv_here
    kv_first = head_index * heads_here // G
    scale = 1.0 / math.sqrt(HD)
    floats = tokens.astype(jnp.float32)
    normed = (
        floats * lax.rsqrt(jnp.mean(floats * floats, axis=1, keepdims=True) + eps_norm) * norm_gain
    ).astype(jnp.bfloat16)
    gathered = lax.all_gather(normed, "head", axis=0, tiled=True)
    key_cols = lax.dynamic_slice_in_dim(w_key, kv_first * HD, kv_here * HD, 1)
    value_cols = lax.dynamic_slice_in_dim(w_value, kv_first * HD, kv_here * HD, 1)
    pieces = (
        lax.all_gather(w_query, "blk", axis=0, tiled=True),
        lax.all_gather(key_cols, "blk", axis=0, tiled=True),
        lax.all_gather(value_cols, "blk", axis=0, tiled=True),
    )
    query_sum, key_sum, value_sum = tuple(
        (jnp.dot(gathered, piece, preferred_element_type=jnp.float32) for piece in pieces)
    )
    positions = block_index * group_rows + jnp.arange(group_rows, dtype=jnp.int32)
    cosine, sine = rotary_tables(positions, HD)
    key_bias_here = lax.dynamic_slice_in_dim(k_bias, kv_first * HD, kv_here * HD, 0)
    value_bias_here = lax.dynamic_slice_in_dim(v_bias, kv_first * HD, kv_here * HD, 0)
    query = rotate((query_sum + q_bias).reshape(group_rows, heads_here, HD), cosine, sine).astype(
        jnp.bfloat16
    )
    grouped = query.reshape(group_rows, kv_here, per_kv, HD)
    keys_here = rotate(
        (key_sum + key_bias_here).reshape(group_rows, kv_here, HD), cosine, sine
    ).astype(jnp.bfloat16)
    keys_here = keys_here.reshape(group_rows, kv_here * HD)
    values_here = (value_sum + value_bias_here).astype(jnp.bfloat16)
    last_query = block_index * group_rows + group_rows - 1
    initial = (
        jnp.full((kv_here, per_kv, group_rows), masked_score, jnp.float32),
        jnp.zeros((kv_here, per_kv, group_rows), jnp.float32),
        jnp.zeros((kv_here, per_kv, group_rows, HD), jnp.float32),
    )
    carry = initial
    pieces = (
        lax.all_gather(keys_here, "blk", axis=0, tiled=True),
        lax.all_gather(values_here, "blk", axis=0, tiled=True),
    )
    rows = pieces[0].shape[0]
    width = block_width(rows, 1024)
    count = rows // width
    key_stack = pieces[0].reshape(count, width, kv_here, HD)
    value_stack = pieces[1].reshape(count, width, kv_here, HD)
    offsets = jnp.arange(count, dtype=jnp.int32) * width

    def step(state, inputs):
        key_block, value_block, key_start = inputs

        def compute(current):
            top, total, acc = current
            scores = (
                jnp.einsum("rgqd,kgd->gqrk", grouped, key_block, preferred_element_type=jnp.float32)
                * scale
            )
            key_positions = key_start + jnp.arange(width, dtype=jnp.int32)
            visible = key_positions[None, :] <= positions[:, None]
            scores = jnp.where(visible, scores, masked_score)
            new_top = jnp.maximum(top, jnp.max(scores, axis=3))
            weights = jnp.where(visible, jnp.exp(scores - new_top[..., None]), 0.0)
            fade = jnp.exp(top - new_top)
            total = total * fade + jnp.sum(weights, axis=3)
            acc = acc * fade[..., None] + jnp.einsum(
                "gqrk,kgd->gqrd",
                weights.astype(jnp.bfloat16),
                value_block,
                preferred_element_type=jnp.float32,
            )
            return (new_top, total, acc)

        def keep(current):
            return current

        return (lax.cond(key_start <= last_query, compute, keep, state), None)

    carry, unused = lax.scan(step, carry, (key_stack, value_stack, offsets))
    top, total, acc = carry
    attended = (
        (acc / total[..., None])
        .transpose(2, 0, 1, 3)
        .reshape(group_rows, heads_here * HD)
        .astype(jnp.bfloat16)
    )
    out_cols = lax.all_gather(w_out, "blk", axis=1, tiled=True)
    return lax.psum_scatter(
        jnp.dot(attended, out_cols, preferred_element_type=jnp.float32).astype(jnp.bfloat16),
        "head",
        scatter_dimension=0,
        tiled=True,
    )


def attend_body(scale, first, q_ref, k_ref, v_ref, qp_ref, kp_ref, o_ref):
    scores = lax.dot_general(
        q_ref[...], k_ref[...], (((1,), (1,)), ((), ())), preferred_element_type=jnp.float32
    )
    visible = kp_ref[...] <= qp_ref[...]
    scores = jnp.where(visible, scores * scale, masked_score)
    top = jnp.max(scores, axis=1, keepdims=True)
    weights = jnp.where(visible, jnp.exp(scores - top), 0.0)
    total = jnp.sum(weights, axis=1, keepdims=True)
    mixed = jnp.dot(weights.astype(jnp.bfloat16), v_ref[...], preferred_element_type=jnp.float32)
    o_ref[...] = (mixed / total).astype(jnp.bfloat16)


def attend(query, keys, values, query_pos, key_pos):
    rows, cols = query.shape
    span = keys.shape[0]
    tile = block_width(rows, 256)
    return pl.pallas_call(
        lambda *refs: attend_body(1.0 / math.sqrt(HD), 0, *refs),
        grid=(rows // tile, cols // HD),
        in_specs=[
            pl.BlockSpec((tile, HD), lambda i, h: (i, h)),
            pl.BlockSpec((span, HD), lambda i, h: (0, 0)),
            pl.BlockSpec((span, HD), lambda i, h: (0, 0)),
            pl.BlockSpec((tile, 1), lambda i, h: (i, 0)),
            pl.BlockSpec((1, span), lambda i, h: (0, 0)),
        ],
        out_specs=pl.BlockSpec((tile, HD), lambda i, h: (i, h)),
        out_shape=jax.ShapeDtypeStruct((rows, cols), jnp.bfloat16),
    )(query, keys, values, query_pos, key_pos)


def on_device(tokens, norm_gain, w_query, w_key, w_value, q_bias, k_bias, v_bias, w_out):
    blocks = lax.axis_size("blk")
    planes = blocks // 4
    x = lax.axis_index("head")
    b = lax.axis_index("blk")
    z, r = b // 4, b % 4
    y, c = r // 2, r % 2
    local_rows, width = tokens.shape
    rows = local_rows * 8
    piece = width // planes
    heads = w_query.shape[1] // HD // 4
    qcols = heads * HD

    def swap(values, bit):
        if bit == 0:
            return lax.ppermute(values, "head", [(0, 1), (1, 0)])
        return lax.ppermute(values, "blk", [(i, i ^ bit) for i in range(blocks)])

    def shift(values, step, wrap=True):
        pairs = [(i, i + 4 * step) for i in range(blocks)]
        if wrap:
            pairs = [(i, j % blocks) for i, j in pairs]
        else:
            pairs = [(i, j) for i, j in pairs if 0 <= j < blocks]
        return lax.ppermute(values, "blk", pairs)

    groups = [[p * 4 + i for i in range(4)] for p in range(planes)]

    def exchange(values):
        return lax.all_to_all(values, "blk", 0, 0, tiled=True, axis_index_groups=groups)

    key_cols = lax.dynamic_slice_in_dim(w_key, x * 2 * HD, 2 * HD, 1)
    value_cols = lax.dynamic_slice_in_dim(w_value, x * 2 * HD, 2 * HD, 1)
    shares = []
    for i in range(4):
        other = key_cols if i % 2 == 0 else value_cols
        g = i // 2
        shares += [w_query[:, i * qcols : (i + 1) * qcols], other[:, g * HD : (g + 1) * HD]]
    share_rows = w_query.shape[0]
    share_cols = qcols + HD
    packed = jnp.concatenate(
        [jnp.concatenate(shares[2 * i : 2 * i + 2], axis=1) for i in range(4)], axis=0
    )
    mine = exchange(packed)
    half = share_cols // 2
    right, left = [mine[:, :half]], [mine[:, half:]]
    for k in range(1, planes):
        right.append(shift(right[-1], 1))
        left.append(shift(left[-1], -1))

    floats = tokens.astype(jnp.float32)
    normed = (
        floats * lax.rsqrt(jnp.mean(floats * floats, axis=1, keepdims=True) + eps_norm) * norm_gain
    ).astype(jnp.bfloat16)
    gathered = jnp.concatenate([normed, swap(normed, 0)], axis=0)
    gathered = jnp.concatenate([gathered, swap(gathered, 2)], axis=0)
    gathered = jnp.concatenate([gathered, swap(gathered, 1)], axis=0)

    def places(core):
        out = []
        for jc in range(2):
            for jy in range(2):
                for jx in range(2):
                    out.append(((y ^ jy) * 2 + (core ^ jc)) * 2 + (x ^ jx))
        starts = jnp.stack(out) * local_rows
        return (starts[:, None] + jnp.arange(local_rows, dtype=jnp.int32)[None, :]).reshape(rows)

    here = places(c)
    positions = z * rows + here
    cosine, sine = rotary_tables(positions, HD)

    out_share = exchange(w_out.reshape(4, qcols, share_rows).reshape(4 * qcols, share_rows))
    out_mine = out_share.reshape(4, qcols, share_rows).transpose(1, 0, 2).reshape(qcols, piece)

    def dot(a, w):
        return jnp.dot(a, w, preferred_element_type=jnp.float32)

    sum_right = sum_left = 0.0
    for k in range(planes):
        sum_right += dot(lax.dynamic_slice_in_dim(gathered, (z - k) % planes * piece, piece, 1), right[k])
        sum_left += dot(lax.dynamic_slice_in_dim(gathered, (z + k) % planes * piece, piece, 1), left[k])
    sums = jnp.concatenate([sum_right, sum_left], axis=1)
    q_part = lax.dynamic_slice_in_dim(q_bias, r * qcols, qcols, 0)
    kv_head = x * 2 + y
    k_part = lax.dynamic_slice_in_dim(k_bias, kv_head * HD, HD, 0)
    v_part = lax.dynamic_slice_in_dim(v_bias, kv_head * HD, HD, 0)
    query = rotate((sums[:, :qcols] + q_part).reshape(rows, heads, HD), cosine, sine)
    query = query.astype(jnp.bfloat16).reshape(rows, qcols)
    as_key = rotate((sums[:, qcols:] + k_part).reshape(rows, 1, HD), cosine, sine).reshape(rows, HD)
    other = jnp.where(c == 0, as_key, sums[:, qcols:] + v_part).astype(jnp.bfloat16)

    parts = [other] + [shift(other, k, wrap=False) for k in range(1, planes)]
    stack = jnp.concatenate(parts, axis=0)
    partner = swap(stack, 1)
    flipped = partner.reshape(planes, 2, rows // 2, HD)[:, ::-1].reshape(planes * rows, HD)
    keys = jnp.where(c == 0, stack, flipped)
    values = jnp.where(c == 0, flipped, stack)
    key_pos = []
    for k in range(planes):
        key_pos.append(jnp.where(z >= k, (z - k) * rows + here, blocks * rows))
    attended = attend(
        query, keys, values, positions[:, None], jnp.concatenate(key_pos)[None, :]
    )

    cut = qcols // 2
    up, down = [out_mine[:cut]], [out_mine[cut:]]
    for k in range(1, planes):
        up.append(shift(up[-1], 1))
        down.append(shift(down[-1], -1))
    pieces = []
    for k in range(planes):
        pieces.append(
            (dot(attended[:, :cut], up[k]) + dot(attended[:, cut:], down[-k % planes])).astype(jnp.bfloat16)
        )

    def fold(kept, sent, bit):
        got = swap(sent, bit)
        return (kept.astype(jnp.float32) + got.astype(jnp.float32)).astype(jnp.bfloat16)

    def halves(v, order):
        n = v.shape[0]
        if order == "x" and n > 2 * local_rows:
            v = v.reshape(2, 2, local_rows, -1)
            return v[:, 0].reshape(n // 2, -1), v[:, 1].reshape(n // 2, -1)
        return v[: n // 2], v[n // 2 :]

    done = []
    for i, column in enumerate(pieces):
        part = fold(*halves(column, "c"), 1)
        if i % 2 == 0:
            part = fold(*halves(part, "y"), 2)
            part = fold(*halves(part, "x"), 0)
        else:
            part = fold(*halves(part, "x"), 0)
            part = fold(*halves(part, "y"), 2)
        done.append(part)
    ordered = jnp.stack(done)
    ordered = jnp.stack([ordered[(z - i) % planes] for i in range(planes)])
    return ordered.transpose(1, 0, 2).reshape(local_rows, width)


def solution(mesh):
    placed = (
        P(("blk", "head"), None),
        P(),
        P("blk", "head"),
        P("blk", None),
        P("blk", None),
        P("head"),
        P(),
        P(),
        P("head", "blk"),
    )
    blocks, head_count = mesh.shape["blk"], mesh.shape["head"]
    fits = blocks % 4 == 0 and head_count == 2

    def body(*args):
        heads_here = args[2].shape[1] // HD
        if fits and heads_here == 2 * G:
            return on_device(*args)
        return on_device_plain(*args)

    return jax.shard_map(
        body, mesh=mesh, in_specs=placed, out_specs=P(("blk", "head"), None), check_vma=False
    )
```

```python
import math

import jax
import jax.numpy as jnp
from jax import lax
from jax.experimental import pallas as pl
from jax.sharding import PartitionSpec as P

HD = 128
G = 6


theta_base = 1000000.0
eps_norm = 1e-06
masked_score = -1e30


def rotary_tables(positions, width):
    half = width // 2
    freq = theta_base ** (-(jnp.arange(half, dtype=jnp.float32) * 2.0 / width))
    angles = positions.astype(jnp.float32)[:, None] * freq[None, :]
    angles = jnp.concatenate([angles, angles], axis=1)
    return (jnp.cos(angles), jnp.sin(angles))


def rotate(values, cosine, sine):
    half = values.shape[-1] // 2
    turned = jnp.concatenate([-values[..., half:], values[..., :half]], axis=-1)
    return values * cosine[:, None, :] + turned * sine[:, None, :]


def block_width(rows, limit):
    width = min(rows, limit)
    while rows % width:
        width -= 1
    return width


def on_device_plain(tokens, norm_gain, w_query, w_key, w_value, q_bias, k_bias, v_bias, w_out):
    head_count = lax.axis_size("head")
    head_index = lax.axis_index("head")
    block_index = lax.axis_index("blk")
    local_rows = tokens.shape[0]
    group_rows = local_rows * head_count
    heads_here = w_query.shape[1] // HD
    kv_here = max(1, heads_here // G)
    per_kv = heads_here // kv_here
    kv_first = head_index * heads_here // G
    scale = 1.0 / math.sqrt(HD)
    floats = tokens.astype(jnp.float32)
    normed = (
        floats * lax.rsqrt(jnp.mean(floats * floats, axis=1, keepdims=True) + eps_norm) * norm_gain
    ).astype(jnp.bfloat16)
    gathered = lax.all_gather(normed, "head", axis=0, tiled=True)
    key_cols = lax.dynamic_slice_in_dim(w_key, kv_first * HD, kv_here * HD, 1)
    value_cols = lax.dynamic_slice_in_dim(w_value, kv_first * HD, kv_here * HD, 1)
    pieces = (
        lax.all_gather(w_query, "blk", axis=0, tiled=True),
        lax.all_gather(key_cols, "blk", axis=0, tiled=True),
        lax.all_gather(value_cols, "blk", axis=0, tiled=True),
    )
    query_sum, key_sum, value_sum = tuple(
        (jnp.dot(gathered, piece, preferred_element_type=jnp.float32) for piece in pieces)
    )
    positions = block_index * group_rows + jnp.arange(group_rows, dtype=jnp.int32)
    cosine, sine = rotary_tables(positions, HD)
    key_bias_here = lax.dynamic_slice_in_dim(k_bias, kv_first * HD, kv_here * HD, 0)
    value_bias_here = lax.dynamic_slice_in_dim(v_bias, kv_first * HD, kv_here * HD, 0)
    query = rotate((query_sum + q_bias).reshape(group_rows, heads_here, HD), cosine, sine).astype(
        jnp.bfloat16
    )
    grouped = query.reshape(group_rows, kv_here, per_kv, HD)
    keys_here = rotate(
        (key_sum + key_bias_here).reshape(group_rows, kv_here, HD), cosine, sine
    ).astype(jnp.bfloat16)
    keys_here = keys_here.reshape(group_rows, kv_here * HD)
    values_here = (value_sum + value_bias_here).astype(jnp.bfloat16)
    last_query = block_index * group_rows + group_rows - 1
    initial = (
        jnp.full((kv_here, per_kv, group_rows), masked_score, jnp.float32),
        jnp.zeros((kv_here, per_kv, group_rows), jnp.float32),
        jnp.zeros((kv_here, per_kv, group_rows, HD), jnp.float32),
    )
    carry = initial
    pieces = (
        lax.all_gather(keys_here, "blk", axis=0, tiled=True),
        lax.all_gather(values_here, "blk", axis=0, tiled=True),
    )
    rows = pieces[0].shape[0]
    width = block_width(rows, 1024)
    count = rows // width
    key_stack = pieces[0].reshape(count, width, kv_here, HD)
    value_stack = pieces[1].reshape(count, width, kv_here, HD)
    offsets = jnp.arange(count, dtype=jnp.int32) * width

    def step(state, inputs):
        key_block, value_block, key_start = inputs

        def compute(current):
            top, total, acc = current
            scores = (
                jnp.einsum("rgqd,kgd->gqrk", grouped, key_block, preferred_element_type=jnp.float32)
                * scale
            )
            key_positions = key_start + jnp.arange(width, dtype=jnp.int32)
            visible = key_positions[None, :] <= positions[:, None]
            scores = jnp.where(visible, scores, masked_score)
            new_top = jnp.maximum(top, jnp.max(scores, axis=3))
            weights = jnp.where(visible, jnp.exp(scores - new_top[..., None]), 0.0)
            fade = jnp.exp(top - new_top)
            total = total * fade + jnp.sum(weights, axis=3)
            acc = acc * fade[..., None] + jnp.einsum(
                "gqrk,kgd->gqrd",
                weights.astype(jnp.bfloat16),
                value_block,
                preferred_element_type=jnp.float32,
            )
            return (new_top, total, acc)

        def keep(current):
            return current

        return (lax.cond(key_start <= last_query, compute, keep, state), None)

    carry, _ = lax.scan(step, carry, (key_stack, value_stack, offsets))
    _, total, acc = carry
    attended = (
        (acc / total[..., None])
        .transpose(2, 0, 1, 3)
        .reshape(group_rows, heads_here * HD)
        .astype(jnp.bfloat16)
    )
    out_cols = lax.all_gather(w_out, "blk", axis=1, tiled=True)
    return lax.psum_scatter(
        jnp.dot(attended, out_cols, preferred_element_type=jnp.float32).astype(jnp.bfloat16),
        "head",
        scatter_dimension=0,
        tiled=True,
    )


def attend_body(scale, q_ref, k_ref, v_ref, qp_ref, kp_ref, o_ref):
    scores = lax.dot_general(
        q_ref[...], k_ref[...], (((1,), (1,)), ((), ())), preferred_element_type=jnp.float32
    )
    visible = kp_ref[...] <= qp_ref[...]
    scores = jnp.where(visible, scores * scale, masked_score)
    top = jnp.max(scores, axis=1, keepdims=True)
    weights = jnp.exp(scores - top)
    total = jnp.sum(weights, axis=1, keepdims=True)
    mixed = jnp.dot(weights.astype(jnp.bfloat16), v_ref[...], preferred_element_type=jnp.float32)
    o_ref[...] = (mixed / total).astype(jnp.bfloat16)


def attend(query, keys, values, query_pos, key_pos):
    rows, cols = query.shape
    span = keys.shape[0]
    tile = block_width(rows, 256)
    return pl.pallas_call(
        lambda *refs: attend_body(1.0 / math.sqrt(HD), *refs),
        grid=(rows // tile, cols // HD),
        in_specs=[
            pl.BlockSpec((tile, HD), lambda i, h: (i, h)),
            pl.BlockSpec((span, HD), lambda i, h: (0, 0)),
            pl.BlockSpec((span, HD), lambda i, h: (0, 0)),
            pl.BlockSpec((tile, 1), lambda i, h: (i, 0)),
            pl.BlockSpec((1, span), lambda i, h: (0, 0)),
        ],
        out_specs=pl.BlockSpec((tile, HD), lambda i, h: (i, h)),
        out_shape=jax.ShapeDtypeStruct((rows, cols), jnp.bfloat16),
    )(query, keys, values, query_pos, key_pos)


def on_device(tokens, norm_gain, w_query, w_key, w_value, q_bias, k_bias, v_bias, w_out):
    CORE, Y, ZL, ZH, X = 1, 2, 4, 8, 0
    blocks = lax.axis_size("blk")
    x = lax.axis_index("head")
    b = lax.axis_index("blk")
    zh, zl, y, c = b // 8, b // 4 % 2, b // 2 % 2, b % 2
    local_rows, width = tokens.shape
    rows = local_rows * 8
    piece = width // 4
    share_rows = w_query.shape[0]
    heads = w_query.shape[1] // HD // 4
    qcols = heads * HD
    share = zl * 2 + c
    kv_head = x * 2 + zl

    def swap(values, bit):
        if bit == X:
            return lax.ppermute(values, "head", [(0, 1), (1, 0)])
        return lax.ppermute(values, "blk", [(i, i ^ bit) for i in range(blocks)])

    groups = [
        [h * 8 + l * 4 + i * 2 + j for l in range(2) for j in range(2)]
        for h in range(2)
        for i in range(2)
    ]

    def exchange(values):
        return lax.all_to_all(values, "blk", 0, 0, tiled=True, axis_index_groups=groups)

    def dot(a, w):
        return jnp.dot(a, w, preferred_element_type=jnp.float32)

    key_cols = lax.dynamic_slice_in_dim(w_key, x * 2 * HD, 2 * HD, 1)
    value_cols = lax.dynamic_slice_in_dim(w_value, x * 2 * HD, 2 * HD, 1)
    shares = []
    for i in range(4):
        other = key_cols if i % 2 == 0 else value_cols
        g = i // 2
        shares.append(
            jnp.concatenate(
                [w_query[:, i * qcols : (i + 1) * qcols], other[:, g * HD : (g + 1) * HD]], axis=1
            )
        )
    mine = exchange(jnp.concatenate(shares, axis=0))
    half = mine.shape[1] // 2
    far = [swap(mine[:, :half], ZH), swap(mine[:, half:], ZH)]
    near = swap(mine, Y)

    floats = tokens.astype(jnp.float32)
    normed = (
        floats * lax.rsqrt(jnp.mean(floats * floats, axis=1, keepdims=True) + eps_norm) * norm_gain
    ).astype(jnp.bfloat16)
    normed = normed.reshape(local_rows, 2, 2, 2, width // 8).transpose(0, 1, 3, 2, 4)
    gathered = normed.reshape(local_rows, width)
    gathered = jnp.concatenate([gathered, swap(gathered, X)], axis=0)
    gathered = jnp.concatenate([gathered, swap(gathered, ZL)], axis=0)
    gathered = jnp.concatenate([gathered, swap(gathered, CORE)], axis=0)

    def places(high, row):
        out = []
        for jc in range(2):
            for jz in range(2):
                for jx in range(2):
                    blk = high * 8 + (zl ^ jz) * 4 + row * 2 + (c ^ jc)
                    out.append(blk * 2 + (x ^ jx))
        starts = jnp.stack(out) * local_rows
        return (starts[:, None] + jnp.arange(local_rows, dtype=jnp.int32)[None, :]).reshape(rows)

    positions = places(zh, y)
    cosine, sine = rotary_tables(positions, HD)

    out_mine = exchange(w_out.reshape(4 * qcols, share_rows))
    out_mine = out_mine.reshape(4, qcols, share_rows).transpose(1, 0, 2).reshape(qcols, piece)
    both = [swap(far[0], Y), swap(far[1], Y)]

    def columns(dz, dy):
        return lax.dynamic_slice_in_dim(gathered, ((zh ^ dz) * 2 + (y ^ dy)) * piece, piece, 1)

    own_cols, near_cols, far_cols, both_cols = columns(0, 0), columns(0, 1), columns(1, 0), columns(1, 1)
    late = [dot(far_cols, far[i]) + dot(both_cols, both[i]) for i in range(2)]
    sums = dot(own_cols, mine) + dot(near_cols, near) + jnp.concatenate(late, axis=1)
    q_part = lax.dynamic_slice_in_dim(q_bias, share * qcols, qcols, 0)
    k_part = lax.dynamic_slice_in_dim(k_bias, kv_head * HD, HD, 0)
    v_part = lax.dynamic_slice_in_dim(v_bias, kv_head * HD, HD, 0)
    as_key = rotate((sums[:, qcols:] + k_part).reshape(rows, 1, HD), cosine, sine).reshape(rows, HD)
    other = jnp.where(c == 0, as_key, sums[:, qcols:] + v_part).astype(jnp.bfloat16)
    other_far = swap(other, ZH)
    stack = [other, swap(other, Y), other_far, swap(other_far, Y)]
    stack = jnp.concatenate(stack, axis=0)
    partner = swap(stack, CORE)
    flipped = partner.reshape(4, 2, rows // 2, HD)[:, ::-1].reshape(4 * rows, HD)
    keys = jnp.where(c == 0, stack, flipped)
    values = jnp.where(c == 0, flipped, stack)
    key_pos = [positions, places(zh, y ^ 1), places(zh ^ 1, y), places(zh ^ 1, y ^ 1)]
    query = rotate((sums[:, :qcols] + q_part).reshape(rows, heads, HD), cosine, sine)
    query = query.astype(jnp.bfloat16).reshape(rows, qcols)
    attended = attend(query, keys, values, positions[:, None], jnp.concatenate(key_pos)[None, :])

    cut = qcols // 2
    out_far = [swap(out_mine[:cut], ZH), swap(out_mine[cut:], ZH)]
    out_near = swap(out_mine, Y)
    out_both = [swap(out_far[0], Y), swap(out_far[1], Y)]

    def project(w):
        if isinstance(w, list):
            return dot(attended[:, :cut], w[0]) + dot(attended[:, cut:], w[1])
        return dot(attended, w)

    def fold(kept, sent, bit):
        got = swap(sent, bit)
        return (kept.astype(jnp.float32) + got.astype(jnp.float32)).astype(jnp.bfloat16)

    def outer(v):
        n = v.shape[0] // 2
        return v[:n], v[n:]

    def inner(v):
        v = v.reshape(2, 2, local_rows, -1)
        return v[:, 0].reshape(2 * local_rows, -1), v[:, 1].reshape(2 * local_rows, -1)

    done = []
    for i, pair in enumerate(((out_mine, out_near), (out_far, out_both))):
        part = jnp.concatenate([project(w).astype(jnp.bfloat16) for w in pair], axis=1)
        part = fold(*outer(part), CORE)
        if i == 0:
            part = fold(*outer(part), ZL)
            part = fold(*outer(part), X)
        else:
            part = fold(*inner(part), X)
            part = fold(*outer(part), ZL)
        done.append(part)
    done = jnp.concatenate(done, axis=1).reshape(local_rows, 2, 2, piece)
    done = jnp.where(y == 0, done, done[:, :, ::-1])
    done = jnp.where(zh == 0, done, done[:, ::-1])
    done = done.reshape(local_rows, 2, 2, 2, width // 8).transpose(0, 1, 3, 2, 4)
    return done.reshape(local_rows, width)


def solution(mesh):
    placed = (
        P(("blk", "head"), None),
        P(),
        P("blk", "head"),
        P("blk", None),
        P("blk", None),
        P("head"),
        P(),
        P(),
        P("head", "blk"),
    )
    blocks, head_count = mesh.shape["blk"], mesh.shape["head"]
    fits = blocks == 16 and head_count == 2

    def body(*args):
        heads_here = args[2].shape[1] // HD
        if fits and heads_here == 2 * G:
            return on_device(*args)
        return on_device_plain(*args)

    return jax.shard_map(
        body, mesh=mesh, in_specs=placed, out_specs=P(("blk", "head"), None), check_vma=False
    )
```
